512 devices in a mesh: groups: 2 (over y), plane: 32 (over z), depth: 4 (over x), tok: 2 (over core).
Axes of the slice: x: 4, y: 2, z: 32, core: 2. Of those that a mesh axis runs over, the one named last changes fastest.
The devices are a block of a 4x8x32 slice.
Arguments:
- tokens: bfloat16 [4096, 2048], P(('groups', 'plane', 'depth', 'tok')), parts along dimension 0, may hold values from -6 to 6
- expert_ids: int32 [4096, 4], P(('groups', 'plane', 'depth', 'tok')), parts along dimension 0, may hold values from 0 to 31, as said below
- slot_index: int32 [4096, 4], P(('groups', 'plane', 'depth', 'tok')), parts along dimension 0, may hold values from 0 to 7, as said below
- route_weight: bfloat16 [4096, 4], P(('groups', 'plane', 'depth', 'tok')), parts along dimension 0, may hold values from 0.099609375 to 1
- shared_gate: bfloat16 [2048], replicated, may hold values from -0.125 to 0.125
- shared_gate_up: bfloat16 [2, 2048, 5632], P(None, None, 'plane'), may hold values from -0.125 to 0.125
- shared_down: bfloat16 [5632, 2048], P('plane'), may hold values from -0.078125 to 0.078125
- expert_gate_up: bfloat16 [32, 2, 2048, 1408], P('plane', None, None, ('depth', 'tok')), may hold values from -0.125 to 0.125
- expert_down: bfloat16 [32, 1408, 2048], P('plane', ('depth', 'tok')), may hold values from -0.15625 to 0.15625
Outputs:
- mixed: bfloat16 [4096, 2048], P(('groups', 'plane', 'depth', 'tok')), parts along dimension 0
The draws below stay inside these ranges and needn't reach their ends.
There are 2 independent parts, one for each index of `groups`. The reference program is written for one: setup_inputs(seed, part) draws one part's arguments, and reference() takes and returns one part's arrays. A program takes and returns all parts, laid end to end along the dimension named above; an argument that names none is the same for every part. Nothing has to cross between parts.
Inputs may be any that keep to these rules, and one draw needn't show every extreme that they name: `expert_ids`: each row names 4 different experts. Among the choices of the rows of one device that name the same expert, slot_index takes each value from 0 to their count minus one exactly once, in an order that varies from draw to draw; the capacity 2 is filled on some devices.
All inputs are finite; a program needn't handle non-finite values.
Results may differ from the reference program's by a relative error of at most 0.019.
Values may be sent and summed in bfloat16 or wider, within the bound.
No kernel may reach another device: no remote copies, remote signals or barrier semaphores. Data moves between devices by JAX's collectives and lax.ppermute only.
A program may use at most 64 MiB of HBM per device.

```python
import math
import jax
import jax.numpy as jnp
from jax import lax

D = 2048
FF_SH = 5632
FF_EX = 1408
TOP = 4
TOK_DEV = 8
TOKENS = 2048
EXPERTS = 32
SHARDS = 8
CAP = 2


def route_table(key):
    base_key = jax.random.fold_in(key, 11)
    first_key, second_key = jax.random.split(base_key)
    order_key = jax.random.fold_in(base_key, 29)
    ranking = jax.random.permutation(first_key, EXPERTS)
    favour = jnp.where(ranking < 4, 256, 0).astype(jnp.int32)
    noise = jax.random.randint(second_key, (TOKENS, EXPERTS), 0, 1024, dtype=jnp.int32)
    scores = (noise + favour[None, :]) * EXPERTS + jnp.arange(EXPERTS, dtype=jnp.int32)[None, :]
    best_values, chosen = lax.top_k(scores, TOP)
    chosen = chosen.astype(jnp.int32)
    entries = TOK_DEV * TOP
    grouped = chosen.reshape(TOKENS // TOK_DEV, entries)
    priority = jax.random.randint(order_key, (TOKENS // TOK_DEV, entries), 0, 1 << 20, dtype=jnp.int32)
    priority = priority * entries + jnp.arange(entries, dtype=jnp.int32)[None, :]
    before = (priority[:, None, :] < priority[:, :, None]).astype(jnp.int32)
    same = (grouped[:, None, :] == grouped[:, :, None]).astype(jnp.int32)
    slots = jnp.sum(before * same, axis=2).reshape(TOKENS, TOP)
    return (chosen, slots.astype(jnp.int32))


def draw_expert_ids(key, part):
    return route_table(key)[0]


def draw_slot_index(key, part):
    return route_table(key)[1]


def block_levels(rng, dims, cuts, smallest, largest):
    factor_of, own = 1.0, jax.random.fold_in(rng, 6)
    for dim, blocks in cuts:
        steps = jnp.exp(jax.random.uniform(jax.random.fold_in(own, dim), (blocks,), jnp.float32, smallest / len(cuts), largest / len(cuts)))
        factor_of = factor_of * jnp.repeat(steps, dims[dim] // blocks).reshape([-1 if axis == dim else 1 for axis in range(len(dims))])
    return factor_of


def gaussian(key, dims, deviation, limit, pieces=(), kind=jnp.bfloat16):
    drawn = deviation * jax.random.normal(key, dims, jnp.float32)
    if pieces:
        drawn = drawn * block_levels(key, dims, pieces, -0.22, 0.18)
    return jnp.clip(drawn, -limit, limit).astype(kind)


def setup_inputs(seed: int = 0, part: int = 0) -> dict:
    key_of = jax.random.split(jax.random.key(seed), 10)
    part_splits = jax.random.split(jax.random.fold_in(key_of[9], part), 10)
    tokens = gaussian(part_splits[0], (TOKENS, D), 1.0, 6.0, ((0, 256),))
    expert_ids = draw_expert_ids(jax.random.fold_in(jax.random.fold_in(key_of[9], part), 71), part)
    slot_index = draw_slot_index(jax.random.fold_in(jax.random.fold_in(key_of[9], part), 71), part)
    route_weight = jnp.clip(jnp.exp(math.log(1.0) - 2.306499 * jax.random.uniform(part_splits[3], (TOKENS, TOP), jnp.float32) ** block_levels(part_splits[3], (TOKENS, TOP), ((0, 256),), -0.2, 0.2)), 0.099609375, 1.0).astype(jnp.bfloat16)
    shared_gate = gaussian(key_of[4], (D,), D ** -0.5, 0.125)
    shared_gate_up = gaussian(key_of[5], (2, D, FF_SH), D ** -0.5, 0.125, ((2, 32),))
    shared_down = gaussian(key_of[6], (FF_SH, D), FF_SH ** -0.5, 0.078125, ((0, 32),))
    expert_gate_up = gaussian(key_of[7], (EXPERTS, 2, D, FF_EX), D ** -0.5, 0.125, ((0, 32), (3, 8)))
    expert_down = gaussian(key_of[8], (EXPERTS, FF_EX, D), FF_EX ** -0.5, 0.15625, ((0, 32), (1, 8)))
    return {"tokens": tokens, "expert_ids": expert_ids, "slot_index": slot_index, "route_weight": route_weight, "shared_gate": shared_gate, "shared_gate_up": shared_gate_up, "shared_down": shared_down, "expert_gate_up": expert_gate_up, "expert_down": expert_down}


def reference(tokens, expert_ids, slot_index, route_weight, shared_gate, shared_gate_up, shared_down, expert_gate_up, expert_down):
    gate_proj = jnp.dot(tokens, shared_gate_up[0], preferred_element_type=jnp.float32)
    up_proj = jnp.dot(tokens, shared_gate_up[1], preferred_element_type=jnp.float32)
    shared_hidden = (jax.nn.silu(gate_proj) * up_proj).astype(jnp.bfloat16)
    shared_out = jnp.dot(shared_hidden, shared_down, preferred_element_type=jnp.float32)
    shared_scale = jax.nn.sigmoid(jnp.dot(tokens, shared_gate, preferred_element_type=jnp.float32))
    blocks = TOKENS // TOK_DEV
    rows_each = blocks * CAP
    token_index = jnp.arange(TOKENS, dtype=jnp.int32)[:, None] + jnp.zeros((1, TOP), jnp.int32)
    kept_mask = slot_index < CAP
    position = expert_ids * rows_each + (token_index // TOK_DEV) * CAP + slot_index
    position = jnp.where(kept_mask, position, EXPERTS * rows_each).reshape(-1)
    source = jnp.zeros((EXPERTS * rows_each,), jnp.int32).at[position].set(token_index.reshape(-1), mode="drop")
    factor = jnp.zeros((EXPERTS * rows_each,), jnp.float32).at[position].set(route_weight.reshape(-1).astype(jnp.float32), mode="drop")
    source = source.reshape(EXPERTS, rows_each)
    factor = factor.reshape(EXPERTS, rows_each)
    block_width = FF_EX // SHARDS

    def one_expert(inputs):
        picked, factor_row, weights_gate_up, weights_down = inputs
        token_rows = tokens[picked]
        gate_part = jnp.dot(token_rows, weights_gate_up[0], preferred_element_type=jnp.float32)
        up_part = jnp.dot(token_rows, weights_gate_up[1], preferred_element_type=jnp.float32)
        hidden = (jax.nn.silu(gate_part) * up_part).astype(jnp.bfloat16)
        partials = jnp.einsum("rsf,sfd->rsd", hidden.reshape(-1, SHARDS, block_width).astype(jnp.float32),
                              weights_down.reshape(SHARDS, block_width, D).astype(jnp.float32),
                              precision=lax.Precision.HIGHEST)
        rounded = lax.optimization_barrier(partials.astype(jnp.bfloat16))
        summed = jnp.sum(rounded.astype(jnp.float32), axis=1)
        return summed * factor_row[:, None]

    contrib = lax.map(one_expert, (source, factor, expert_gate_up, expert_down))
    routed = jnp.zeros((TOKENS, D), jnp.float32).at[source.reshape(-1)].add(contrib.reshape(-1, D))
    return (shared_scale[:, None] * shared_out + routed).astype(jnp.bfloat16)
```

```python
import jax
import jax.numpy as jnp
from jax import lax
from jax.sharding import PartitionSpec as P

LANES = 128


def from_offset(block, axis, offset):
    size = lax.axis_size(axis)
    return lax.ppermute(block, axis, [((i + offset) % size, i) for i in range(size)])


def far_groups(planes, near):
    return [[r + near * f for f in range(planes // near)] for r in range(near)]


def gather_planes(block, near):
    planes = lax.axis_size("plane")
    own = lax.all_gather(block, "plane", axis_index_groups=far_groups(planes, near))
    half = own.shape[0] // 2
    up = from_offset(own, "plane", 1)
    down = from_offset(own, "plane", -1)
    low = from_offset(own[:half], "plane", 2)
    high = from_offset(own[half:], "plane", -2)
    return jnp.stack([own, up, jnp.concatenate([low, high]), down])


def reduce_planes(blocks, near):
    planes = lax.axis_size("plane")
    sent = blocks.astype(jnp.bfloat16)
    half = blocks.shape[1] // 2
    up = from_offset(sent[1], "plane", -1)
    down = from_offset(sent[3], "plane", 1)
    low = from_offset(sent[2, :half], "plane", -2)
    high = from_offset(sent[2, half:], "plane", 2)
    total = blocks[0] + up.astype(jnp.float32) + down.astype(jnp.float32)
    total = total + jnp.concatenate([low, high]).astype(jnp.float32)
    arrived = lax.all_to_all(
        total.astype(jnp.bfloat16),
        "plane",
        split_axis=0,
        concat_axis=0,
        tiled=True,
        axis_index_groups=far_groups(planes, near),
    )
    return arrived.astype(jnp.float32).sum(axis=0)


def gather_rows(rows):
    depth = lax.axis_size("depth")
    column = jnp.stack([rows] + [from_offset(rows, "depth", k) for k in range(1, depth)])
    return jnp.stack([column, from_offset(column, "tok", 1)])


def reduce_rows(partials):
    depth = lax.axis_size("depth")
    swapped = from_offset(partials[1], "tok", 1)
    column = partials[0].astype(jnp.float32) + swapped.astype(jnp.float32)
    sent = column.astype(jnp.bfloat16)
    total = column[0]
    for k in range(1, depth):
        total = total + from_offset(sent[k], "depth", -k).astype(jnp.float32)
    return total


def gated_rows(token_rows, gate_up):
    gate_part = jnp.dot(token_rows, gate_up[0], preferred_element_type=jnp.float32)
    up_part = jnp.dot(token_rows, gate_up[1], preferred_element_type=jnp.float32)
    return (jax.nn.silu(gate_part) * up_part).astype(jnp.bfloat16)


def on_device(
    tokens,
    expert_ids,
    slot_index,
    route_weight,
    shared_gate,
    shared_gate_up,
    shared_down,
    expert_gate_up,
    expert_down,
):
    planes = lax.axis_size("plane")
    tok_rows, width = tokens.shape
    choices = expert_ids.shape[1]
    capacity = max(2, tok_rows * choices // planes)
    near = 4
    slots = planes * capacity

    code = jnp.where(slot_index < capacity, expert_ids * capacity + slot_index, -1)
    notes = jnp.concatenate([code.astype(jnp.bfloat16), route_weight], axis=1)
    notes = jnp.pad(notes, ((0, 0), (0, LANES - 2 * choices)))
    gathered = gather_planes(jnp.concatenate([tokens, notes], axis=1), near)
    gathered = gathered.reshape(planes * tok_rows, width + LANES)
    all_tokens = gathered[:, :width]
    codes = gathered[:, width : width + choices].astype(jnp.float32)
    weights = gathered[:, width + choices : width + 2 * choices].astype(jnp.float32)

    mine = (lax.axis_index("plane") * capacity).astype(jnp.float32)
    count = planes * tok_rows
    here = lax.broadcasted_iota(jnp.int32, (count, slots), 0) // tok_rows
    column = lax.broadcasted_iota(jnp.int32, (count, slots), 1)
    slot_code = mine + (column % capacity).astype(jnp.float32)
    hit = jnp.any(codes[:, None, :] == slot_code[:, :, None], axis=2)
    pick = (hit & (here == column // capacity)).astype(jnp.bfloat16)
    matched = (codes >= mine) & (codes < mine + capacity)
    factor = jnp.sum(jnp.where(matched, weights, 0.0), axis=1, keepdims=True)

    rows = lax.dot_general(
        pick, all_tokens, (((0,), (0,)), ((), ())), preferred_element_type=jnp.float32
    ).astype(jnp.bfloat16)
    expert_in = gather_rows(rows)
    shape = expert_in.shape
    hidden = gated_rows(expert_in.reshape(-1, width), expert_gate_up[0])
    partials = jnp.dot(hidden, expert_down[0], preferred_element_type=jnp.float32)
    expert_out = reduce_rows(partials.astype(jnp.bfloat16).reshape(shape))

    shared_hidden = gated_rows(all_tokens, shared_gate_up)
    shared_part = jnp.dot(shared_hidden, shared_down, preferred_element_type=jnp.float32)
    shared_scale = jax.nn.sigmoid(
        jnp.dot(all_tokens, shared_gate, preferred_element_type=jnp.float32)
    )
    routed = jnp.dot(pick, expert_out.astype(jnp.bfloat16), preferred_element_type=jnp.float32)
    share = shared_scale[:, None] * shared_part + factor * routed
    share = share.reshape(near, planes // near, tok_rows, width)
    return reduce_planes(share, near).astype(jnp.bfloat16)


def solution(mesh):
    in_specs = (
        P(("groups", "plane", "depth", "tok"), None),
        P(("groups", "plane", "depth", "tok"), None),
        P(("groups", "plane", "depth", "tok"), None),
        P(("groups", "plane", "depth", "tok"), None),
        P(),
        P(None, None, "plane"),
        P("plane", None),
        P("plane", None, None, ("depth", "tok")),
        P("plane", ("depth", "tok"), None),
    )
    out_specs = P(("groups", "plane", "depth", "tok"), None)
    return jax.shard_map(
        on_device, mesh=mesh, in_specs=in_specs, out_specs=out_specs, check_vma=False
    )
```

```python
import jax
import jax.numpy as jnp
from jax import lax
from jax.sharding import PartitionSpec as P

LANES = 128


def from_offset(block, axis, offset):
    size = lax.axis_size(axis)
    return lax.ppermute(block, axis, [((i + offset) % size, i) for i in range(size)])


def far_groups(planes, near):
    return [[r + near * f for f in range(planes // near)] for r in range(near)]


def gather_planes(block, near):
    planes = lax.axis_size("plane")
    own = lax.all_gather(block, "plane", axis_index_groups=far_groups(planes, near))
    half = own.shape[0] // 2
    low = from_offset(own[:half], "plane", 2)
    high = from_offset(own[half:], "plane", -2)
    up = from_offset(own, "plane", 1)
    down = from_offset(own, "plane", -1)
    return jnp.stack([own, up, jnp.concatenate([low, high]), down])


def reduce_planes(blocks, near):
    planes = lax.axis_size("plane")
    sent = blocks.astype(jnp.bfloat16)
    half = blocks.shape[1] // 2
    up = from_offset(sent[1], "plane", -1)
    down = from_offset(sent[3], "plane", 1)
    low = from_offset(sent[2, :half], "plane", -2)
    high = from_offset(sent[2, half:], "plane", 2)
    total = blocks[0] + up.astype(jnp.float32) + down.astype(jnp.float32)
    total = total + jnp.concatenate([low, high]).astype(jnp.float32)
    arrived = lax.all_to_all(
        total.astype(jnp.bfloat16),
        "plane",
        split_axis=0,
        concat_axis=0,
        tiled=True,
        axis_index_groups=far_groups(planes, near),
    )
    return arrived.astype(jnp.float32).sum(axis=0)


def gather_rows(rows):
    depth = lax.axis_size("depth")
    return jnp.stack([rows] + [from_offset(rows, "depth", k) for k in range(1, depth)])


def reduce_rows(partials):
    depth = lax.axis_size("depth")
    sent = partials.astype(jnp.bfloat16)
    total = partials[0]
    for k in range(1, depth):
        total = total + from_offset(sent[k], "depth", -k).astype(jnp.float32)
    return total


def chip_shards(shard):
    return [shard] + [from_offset(shard, "tok", k) for k in range(1, lax.axis_size("tok"))]


def gated_rows(token_rows, gate_up):
    gate_part = jnp.dot(token_rows, gate_up[0], preferred_element_type=jnp.float32)
    up_part = jnp.dot(token_rows, gate_up[1], preferred_element_type=jnp.float32)
    return lax.optimization_barrier((jax.nn.silu(gate_part) * up_part).astype(jnp.bfloat16))


def on_device(
    tokens,
    expert_ids,
    slot_index,
    route_weight,
    shared_gate,
    shared_gate_up,
    shared_down,
    expert_gate_up,
    expert_down,
):
    planes = lax.axis_size("plane")
    tok_rows, width = tokens.shape
    choices = expert_ids.shape[1]
    capacity = max(2, tok_rows * choices // planes)
    near = 4
    slots = planes * capacity

    code = jnp.where(slot_index < capacity, expert_ids * capacity + slot_index, -1)
    notes = jnp.concatenate([code.astype(jnp.bfloat16), route_weight], axis=1)
    notes = jnp.pad(notes, ((0, 0), (0, LANES - 2 * choices)))
    gathered = gather_planes(jnp.concatenate([tokens, notes], axis=1), near)
    gathered = gathered.reshape(planes * tok_rows, width + LANES)
    all_tokens = gathered[:, :width]
    codes = gathered[:, width : width + choices].astype(jnp.float32)
    weights = gathered[:, width + choices : width + 2 * choices].astype(jnp.float32)

    mine = (lax.axis_index("plane") * capacity).astype(jnp.float32)
    count = planes * tok_rows
    here = lax.broadcasted_iota(jnp.int32, (count, slots), 0) // tok_rows
    column = lax.broadcasted_iota(jnp.int32, (count, slots), 1)
    slot_code = mine + (column % capacity).astype(jnp.float32)
    hit = jnp.any(codes[:, None, :] == slot_code[:, :, None], axis=2)
    pick = (hit & (here == column // capacity)).astype(jnp.bfloat16)
    pick = lax.optimization_barrier(pick)
    matched = (codes >= mine) & (codes < mine + capacity)
    factor = jnp.sum(jnp.where(matched, weights, 0.0), axis=1, keepdims=True)

    rows = lax.dot_general(
        pick, all_tokens, (((0,), (0,)), ((), ())), preferred_element_type=jnp.float32
    ).astype(jnp.bfloat16)
    expert_in = gather_rows(rows)
    shape = expert_in.shape
    flat = expert_in.reshape(-1, width)
    partials = jnp.zeros((), jnp.float32)
    for gate_up, down in zip(chip_shards(expert_gate_up[0]), chip_shards(expert_down[0])):
        hidden = gated_rows(flat, gate_up)
        partials = partials + jnp.dot(hidden, down, preferred_element_type=jnp.float32)
    expert_out = reduce_rows(partials.reshape(shape))

    shared_hidden = gated_rows(all_tokens, shared_gate_up)
    shared_part = jnp.dot(shared_hidden, shared_down, preferred_element_type=jnp.float32)
    shared_scale = jax.nn.sigmoid(
        jnp.dot(all_tokens, shared_gate, preferred_element_type=jnp.float32)
    )
    routed = jnp.dot(pick, expert_out.astype(jnp.bfloat16), preferred_element_type=jnp.float32)
    share = shared_scale[:, None] * shared_part + factor * routed
    share = share.reshape(near, planes // near, tok_rows, width)
    return reduce_planes(share, near).astype(jnp.bfloat16)


def solution(mesh):
    in_specs = (
        P(("groups", "plane", "depth", "tok"), None),
        P(("groups", "plane", "depth", "tok"), None),
        P(("groups", "plane", "depth", "tok"), None),
        P(("groups", "plane", "depth", "tok"), None),
        P(),
        P(None, None, "plane"),
        P("plane", None),
        P("plane", None, None, ("depth", "tok")),
        P("plane", ("depth", "tok"), None),
    )
    out_specs = P(("groups", "plane", "depth", "tok"), None)
    return jax.shard_map(
        on_device, mesh=mesh, in_specs=in_specs, out_specs=out_specs, check_vma=False
    )
```

```python
import jax
import jax.numpy as jnp
import numpy as np
from jax import lax
from jax.sharding import PartitionSpec as P

LANES = 128


def from_offset(block, axis, offset):
    size = lax.axis_size(axis)
    return lax.ppermute(block, axis, [((i + offset) % size, i) for i in range(size)])


def far_groups(planes, near):
    return [[r + near * f for f in range(planes // near)] for r in range(near)]


def gather_far(block, near):
    groups = far_groups(lax.axis_size("plane"), near)
    return lax.all_gather(block, "plane", axis_index_groups=groups)


def scatter_far(sums, near):
    arrived = lax.all_to_all(
        sums.astype(jnp.bfloat16),
        "plane",
        split_axis=0,
        concat_axis=0,
        tiled=True,
        axis_index_groups=far_groups(lax.axis_size("plane"), near),
    )
    return arrived.astype(jnp.float32).sum(axis=0)


def gather_near(own):
    half = own.shape[0] // 2
    up = from_offset(own, "plane", 1)
    down = from_offset(own, "plane", -1)
    low = from_offset(own[:half], "plane", 2)
    high = from_offset(own[half:], "plane", -2)
    return jnp.stack([own, up, jnp.concatenate([low, high]), down])


def reduce_near(parts):
    sent = parts.astype(jnp.bfloat16)
    half = parts.shape[1] // 2
    up = from_offset(sent[1], "plane", -1)
    down = from_offset(sent[3], "plane", 1)
    low = from_offset(sent[2, :half], "plane", -2)
    high = from_offset(sent[2, half:], "plane", 2)
    total = parts[0] + up.astype(jnp.float32) + down.astype(jnp.float32)
    return total + jnp.concatenate([low, high]).astype(jnp.float32)


def slot_columns(classes, capacity):
    half = classes // 2
    spans = ((0, 0, classes), (-1, 0, classes), (1, 0, classes), (-2, 0, half), (2, half, classes))
    table = [(k, f, s) for k, a, b in spans for f in range(a, b) for s in range(capacity)]
    return [np.array(column, np.int32) for column in zip(*table)]


def gather_rows(rows):
    depth = lax.axis_size("depth")
    return jnp.stack([rows] + [from_offset(rows, "depth", k) for k in range(1, depth)])


def reduce_rows(partials):
    depth = lax.axis_size("depth")
    sent = partials.astype(jnp.bfloat16)
    total = partials[0]
    for k in range(1, depth):
        arrived = from_offset(sent[k], "depth", -k)
        total = total + arrived.astype(jnp.float32)
    return total


def chip_shards(shard):
    return [shard] + [from_offset(shard, "tok", k) for k in range(1, lax.axis_size("tok"))]


def gated_rows(token_rows, gate_up):
    gate_part = jnp.dot(token_rows, gate_up[0], preferred_element_type=jnp.float32)
    up_part = jnp.dot(token_rows, gate_up[1], preferred_element_type=jnp.float32)
    return lax.optimization_barrier((jax.nn.silu(gate_part) * up_part).astype(jnp.bfloat16))


def on_device(
    tokens,
    expert_ids,
    slot_index,
    route_weight,
    shared_gate,
    shared_gate_up,
    shared_down,
    expert_gate_up,
    expert_down,
):
    planes = lax.axis_size("plane")
    tok_rows, width = tokens.shape
    choices = expert_ids.shape[1]
    capacity = max(2, tok_rows * choices // planes)
    near = 4
    classes = planes // near
    count = classes * tok_rows
    full = classes * capacity
    half = full // 2

    code = jnp.where(slot_index < capacity, expert_ids * capacity + slot_index, -1)
    notes = jnp.concatenate([code.astype(jnp.bfloat16), route_weight], axis=1)
    notes = jnp.pad(notes, ((0, 0), (0, LANES - 2 * choices)))
    gathered = gather_far(jnp.concatenate([tokens, notes], axis=1), near)
    gathered = gathered.reshape(count, width + LANES)
    own_tokens = gathered[:, :width]
    codes = gathered[:, width : width + choices].astype(jnp.float32)
    weights = gathered[:, width + choices : width + 2 * choices].astype(jnp.float32)

    offset, place, slot = slot_columns(classes, capacity)
    expert = jnp.mod(lax.axis_index("plane") + offset, planes)
    wanted = (expert * capacity + slot).astype(jnp.float32)
    here = (np.arange(count)[:, None] // tok_rows) == place[None, :]
    matches = (codes[:, None, :] == wanted[None, :, None]) & here[:, :, None]
    pick = jnp.any(matches, axis=2).astype(jnp.bfloat16)
    mix = jnp.sum(jnp.where(matches, weights[:, None, :], 0.0), axis=2).astype(jnp.bfloat16)
    pick, mix = lax.optimization_barrier((pick, mix))

    rows = lax.dot_general(
        pick, own_tokens, (((0,), (0,)), ((), ())), preferred_element_type=jnp.float32
    ).astype(jnp.bfloat16)
    up = from_offset(rows[full : 2 * full], "plane", 1)
    down = from_offset(rows[2 * full : 3 * full], "plane", -1)
    low = from_offset(rows[3 * full : 3 * full + half], "plane", 2)
    high = from_offset(rows[3 * full + half :], "plane", -2)
    expert_rows = jnp.concatenate([rows[:full], up, low, high, down])
    expert_rows, own_tokens = lax.optimization_barrier((expert_rows, own_tokens))
    expert_in = gather_rows(expert_rows)
    all_tokens = gather_near(own_tokens.reshape(classes, tok_rows, width))

    flat = expert_in.reshape(-1, width)
    partials = jnp.zeros((), jnp.float32)
    for gate_up, down_proj in zip(chip_shards(expert_gate_up[0]), chip_shards(expert_down[0])):
        hidden = gated_rows(flat, gate_up)
        partials = partials + jnp.dot(hidden, down_proj, preferred_element_type=jnp.float32)
    expert_out = reduce_rows(partials.reshape(expert_in.shape)).astype(jnp.bfloat16)

    shared_hidden = gated_rows(all_tokens.reshape(-1, width), shared_gate_up)
    shared_part = jnp.dot(shared_hidden, shared_down, preferred_element_type=jnp.float32)
    shared_out = reduce_near(shared_part.reshape(all_tokens.shape)).reshape(count, width)
    shared_scale = jax.nn.sigmoid(
        jnp.dot(own_tokens, shared_gate, preferred_element_type=jnp.float32)
    )

    up = from_offset(expert_out[full : 2 * full], "plane", -1)
    low = from_offset(expert_out[2 * full : 2 * full + half], "plane", -2)
    high = from_offset(expert_out[2 * full + half : 3 * full], "plane", 2)
    down = from_offset(expert_out[3 * full :], "plane", 1)
    returned = jnp.concatenate([expert_out[:full], up, down, low, high])
    routed = jnp.dot(mix, returned, preferred_element_type=jnp.float32)
    total = shared_scale[:, None] * shared_out + routed
    return scatter_far(total.reshape(classes, tok_rows, width), near).astype(jnp.bfloat16)


def solution(mesh):
    in_specs = (
        P(("groups", "plane", "depth", "tok"), None),
        P(("groups", "plane", "depth", "tok"), None),
        P(("groups", "plane", "depth", "tok"), None),
        P(("groups", "plane", "depth", "tok"), None),
        P(),
        P(None, None, "plane"),
        P("plane", None),
        P("plane", None, None, ("depth", "tok")),
        P("plane", ("depth", "tok"), None),
    )
    out_specs = P(("groups", "plane", "depth", "tok"), None)
    return jax.shard_map(
        on_device, mesh=mesh, in_specs=in_specs, out_specs=out_specs, check_vma=False
    )
```

```python
import jax
import jax.numpy as jnp
from jax import lax
from jax.sharding import PartitionSpec as P

LANES = 128


def from_offset(block, axis, offset):
    size, cores = lax.axis_size(axis), lax.axis_size("tok")
    pairs = [
        (((i + (-offset if t % 2 else offset)) % size) * cores + t, i * cores + t)
        for i in range(size)
        for t in range(cores)
    ]
    return lax.ppermute(block, (axis, "tok"), pairs)


def from_core(block, offset):
    size = lax.axis_size("tok")
    return lax.ppermute(block, "tok", [((i + offset) % size, i) for i in range(size)])


def far_groups(planes, near):
    return [[r + near * f for f in range(planes // near)] for r in range(near)]


def gather_planes(block, near):
    groups = far_groups(lax.axis_size("plane"), near)
    own = lax.all_gather(block, "plane", axis_index_groups=groups)
    return jnp.stack([own] + [from_offset(own, "plane", k) for k in (1, 2, -1)])


def reduce_planes(blocks, near):
    sent = blocks.astype(jnp.bfloat16)
    total = blocks[0]
    for j, k in ((1, 1), (2, 2), (3, -1)):
        total = total + from_offset(sent[j], "plane", -k).astype(jnp.float32)
    arrived = lax.all_to_all(
        total.astype(jnp.bfloat16),
        "plane",
        split_axis=0,
        concat_axis=0,
        tiled=True,
        axis_index_groups=far_groups(lax.axis_size("plane"), near),
    )
    return arrived.astype(jnp.float32).sum(axis=0)


def gather_rows(rows):
    return jnp.stack([rows] + [from_offset(rows, "depth", k) for k in (1, -1, 2)])


def reduce_rows(partials):
    sent = partials.astype(jnp.bfloat16)
    total = partials[0]
    for j, k in ((1, 1), (2, -1), (3, 2)):
        total = total + from_offset(sent[j], "depth", -k).astype(jnp.float32)
    return total


def chip_shards(shard):
    return [shard] + [from_core(shard, k) for k in range(1, lax.axis_size("tok"))]


def gated_rows(token_rows, gate_up):
    gate_part = jnp.dot(token_rows, gate_up[0], preferred_element_type=jnp.float32)
    up_part = jnp.dot(token_rows, gate_up[1], preferred_element_type=jnp.float32)
    return lax.optimization_barrier((jax.nn.silu(gate_part) * up_part).astype(jnp.bfloat16))


def on_device(
    tokens,
    expert_ids,
    slot_index,
    route_weight,
    shared_gate,
    shared_gate_up,
    shared_down,
    expert_gate_up,
    expert_down,
):
    planes = lax.axis_size("plane")
    tok_rows, width = tokens.shape
    choices = expert_ids.shape[1]
    capacity = max(2, tok_rows * choices // planes)
    near = 4
    slots = planes * capacity

    code = jnp.where(slot_index < capacity, expert_ids * capacity + slot_index, -1)
    notes = jnp.concatenate([code.astype(jnp.bfloat16), route_weight], axis=1)
    notes = jnp.pad(notes, ((0, 0), (0, LANES - 2 * choices)))
    gathered = gather_planes(jnp.concatenate([tokens, notes], axis=1), near)
    gathered = gathered.reshape(planes * tok_rows, width + LANES)
    all_tokens = gathered[:, :width]
    codes = gathered[:, width : width + choices].astype(jnp.float32)
    weights = gathered[:, width + choices : width + 2 * choices].astype(jnp.float32)

    mine = (lax.axis_index("plane") * capacity).astype(jnp.float32)
    count = planes * tok_rows
    here = lax.broadcasted_iota(jnp.int32, (count, slots), 0) // tok_rows
    column = lax.broadcasted_iota(jnp.int32, (count, slots), 1)
    slot_code = mine + (column % capacity).astype(jnp.float32)
    hit = jnp.any(codes[:, None, :] == slot_code[:, :, None], axis=2)
    pick = (hit & (here == column // capacity)).astype(jnp.bfloat16)
    pick = lax.optimization_barrier(pick)
    matched = (codes >= mine) & (codes < mine + capacity)
    factor = jnp.sum(jnp.where(matched, weights, 0.0), axis=1, keepdims=True)

    rows = lax.dot_general(
        pick, all_tokens, (((0,), (0,)), ((), ())), preferred_element_type=jnp.float32
    ).astype(jnp.bfloat16)
    expert_in = gather_rows(rows)
    shape = expert_in.shape
    flat = expert_in.reshape(-1, width)
    partials = jnp.zeros((), jnp.float32)
    for gate_up, down in zip(chip_shards(expert_gate_up[0]), chip_shards(expert_down[0])):
        hidden = gated_rows(flat, gate_up)
        partials = partials + jnp.dot(hidden, down, preferred_element_type=jnp.float32)
    expert_out = reduce_rows(partials.reshape(shape))

    shared_hidden = gated_rows(all_tokens, shared_gate_up)
    shared_part = jnp.dot(shared_hidden, shared_down, preferred_element_type=jnp.float32)
    shared_scale = jax.nn.sigmoid(
        jnp.dot(all_tokens, shared_gate, preferred_element_type=jnp.float32)
    )
    routed = jnp.dot(pick, expert_out.astype(jnp.bfloat16), preferred_element_type=jnp.float32)
    share = shared_scale[:, None] * shared_part + factor * routed
    share = share.reshape(near, planes // near, tok_rows, width)
    return reduce_planes(share, near).astype(jnp.bfloat16)


def solution(mesh):
    in_specs = (
        P(("groups", "plane", "depth", "tok"), None),
        P(("groups", "plane", "depth", "tok"), None),
        P(("groups", "plane", "depth", "tok"), None),
        P(("groups", "plane", "depth", "tok"), None),
        P(),
        P(None, None, "plane"),
        P("plane", None),
        P("plane", None, None, ("depth", "tok")),
        P("plane", ("depth", "tok"), None),
    )
    out_specs = P(("groups", "plane", "depth", "tok"), None)
    return jax.shard_map(
        on_device, mesh=mesh, in_specs=in_specs, out_specs=out_specs, check_vma=False
    )
```

```python
import jax
import jax.numpy as jnp
from jax import lax
from jax.experimental import pallas as pl
from jax.experimental.pallas import tpu as pltpu
from jax.sharding import PartitionSpec as P

LANES = 128
KERNEL_VMEM = 14 << 20


def from_offset(block, axis, offset):
    size, cores = lax.axis_size(axis), lax.axis_size("tok")
    pairs = [
        (((i + (-offset if t % 2 else offset)) % size) * cores + t, i * cores + t)
        for i in range(size)
        for t in range(cores)
    ]
    return lax.ppermute(block, (axis, "tok"), pairs)


def from_core(block):
    size = lax.axis_size("tok")
    return lax.ppermute(block, "tok", [((i + 1) % size, i) for i in range(size)])


def far_groups(planes, near):
    return [[r + near * f for f in range(planes // near)] for r in range(near)]


def gather_planes(block, near):
    groups = far_groups(lax.axis_size("plane"), near)
    own = lax.all_gather(block, "plane", axis_index_groups=groups)
    return jnp.stack([own] + [from_offset(own, "plane", k) for k in (1, 2, -1)])


def reduce_planes(blocks, near):
    sent = blocks.astype(jnp.bfloat16)
    total = blocks[0]
    for j, k in ((1, 1), (2, 2), (3, -1)):
        total = total + from_offset(sent[j], "plane", -k).astype(jnp.float32)
    arrived = lax.all_to_all(
        total.astype(jnp.bfloat16),
        "plane",
        split_axis=0,
        concat_axis=0,
        tiled=True,
        axis_index_groups=far_groups(lax.axis_size("plane"), near),
    )
    return arrived.astype(jnp.float32).sum(axis=0)


def from_chip(block, partner):
    size = lax.axis_size("depth")
    return lax.ppermute(block, "depth", [(partner(i, size), i) for i in range(size)])


def weight_partner(place, size):
    return place ^ 1


def row_partner(place, size):
    return size - 1 - place


def expert_kernel(own_ref, other_ref, *refs):
    shards = (len(refs) - 5) // 2
    gate_up_refs, down_refs = refs[:shards], refs[shards : 2 * shards]
    kept_ref, sent_ref, gate_up, down, sems = refs[2 * shards :]
    copies = []
    for s in range(shards):
        copies.append(pltpu.make_async_copy(gate_up_refs[s], gate_up.at[s], sems.at[2 * s]))
        copies.append(pltpu.make_async_copy(down_refs[s], down.at[s], sems.at[2 * s + 1]))
    for copy in copies:
        copy.start()
    rows = jnp.concatenate([own_ref[...], other_ref[...]])
    contract = (((1,), (1,)), ((), ()))
    total = None
    for s in range(shards):
        copies[2 * s].wait()
        gate = lax.dot_general(rows, gate_up[s, 0], contract, preferred_element_type=jnp.float32)
        up = lax.dot_general(rows, gate_up[s, 1], contract, preferred_element_type=jnp.float32)
        hidden = (gate / (1.0 + jnp.exp(-gate)) * up).astype(jnp.bfloat16)
        copies[2 * s + 1].wait()
        part = jnp.dot(hidden, down[s], preferred_element_type=jnp.float32)
        total = part if total is None else total + part
    half = own_ref.shape[0]
    kept_ref[...] = total[:half]
    sent_ref[...] = total[half:].astype(jnp.bfloat16)


def expert_partials(own, other, gate_ups, downs):
    rows, width = own.shape
    units = downs[0].shape[0]
    vmem, anywhere = pl.BlockSpec(memory_space=pltpu.VMEM), pl.BlockSpec(memory_space=pl.ANY)
    shards = len(downs)
    return pl.pallas_call(
        expert_kernel,
        out_shape=(
            jax.ShapeDtypeStruct((rows, width), jnp.float32),
            jax.ShapeDtypeStruct((rows, width), jnp.bfloat16),
        ),
        in_specs=[vmem, vmem] + [anywhere] * (2 * shards),
        out_specs=(vmem, vmem),
        scratch_shapes=[
            pltpu.VMEM((shards, 2, units, width), jnp.bfloat16),
            pltpu.VMEM((shards, units, width), jnp.bfloat16),
            pltpu.SemaphoreType.DMA((2 * shards,)),
        ],
        compiler_params=pltpu.CompilerParams(vmem_limit_bytes=KERNEL_VMEM),
        cost_estimate=pl.CostEstimate(
            flops=12 * shards * rows * width * units,
            bytes_accessed=6 * shards * units * width,
            transcendentals=2 * shards * rows * units,
        ),
    )(own, other, *gate_ups, *downs)


def gated_rows(token_rows, gate_up):
    gate_part = jnp.dot(token_rows, gate_up[0], preferred_element_type=jnp.float32)
    up_part = jnp.dot(token_rows, gate_up[1], preferred_element_type=jnp.float32)
    return lax.optimization_barrier((jax.nn.silu(gate_part) * up_part).astype(jnp.bfloat16))


def on_device(
    tokens,
    expert_ids,
    slot_index,
    route_weight,
    shared_gate,
    shared_gate_up,
    shared_down,
    expert_gate_up,
    expert_down,
):
    planes = lax.axis_size("plane")
    tok_rows, width = tokens.shape
    choices = expert_ids.shape[1]
    capacity = max(2, tok_rows * choices // planes)
    near = 4
    slots = planes * capacity

    code = jnp.where(slot_index < capacity, expert_ids * capacity + slot_index, -1)
    notes = jnp.concatenate([code.astype(jnp.bfloat16), route_weight], axis=1)
    notes = jnp.pad(notes, ((0, 0), (0, LANES - 2 * choices)))
    gathered = gather_planes(jnp.concatenate([tokens, notes], axis=1), near)
    gathered = gathered.reshape(planes * tok_rows, width + LANES)
    all_tokens = gathered[:, :width]
    codes = gathered[:, width : width + choices].astype(jnp.float32)
    weights = gathered[:, width + choices : width + 2 * choices].astype(jnp.float32)

    mine = (lax.axis_index("plane") * capacity).astype(jnp.float32)
    count = planes * tok_rows
    here = lax.broadcasted_iota(jnp.int32, (count, slots), 0) // tok_rows
    column = lax.broadcasted_iota(jnp.int32, (count, slots), 1)
    slot_code = mine + (column % capacity).astype(jnp.float32)
    hit = jnp.any(codes[:, None, :] == slot_code[:, :, None], axis=2)
    pick = (hit & (here == column // capacity)).astype(jnp.bfloat16)
    pick = lax.optimization_barrier(pick)
    matched = (codes >= mine) & (codes < mine + capacity)
    factor = jnp.sum(jnp.where(matched, weights, 0.0), axis=1, keepdims=True)

    rows = lax.dot_general(
        pick, all_tokens, (((0,), (0,)), ((), ())), preferred_element_type=jnp.float32
    ).astype(jnp.bfloat16)
    gate_up, down = expert_gate_up[0].swapaxes(1, 2), expert_down[0]
    gate_up_chip = from_chip(gate_up, weight_partner)
    down_chip = from_chip(down, weight_partner)
    gate_up_core, down_core = from_core(gate_up), from_core(down)
    gate_up_far = from_core(gate_up_chip)
    down_far = from_core(down_chip)
    other_rows = from_chip(rows, row_partner)
    kept, sent = expert_partials(
        rows,
        other_rows,
        (gate_up, gate_up_core, gate_up_chip, gate_up_far),
        (down, down_core, down_chip, down_far),
    )
    shared_hidden = gated_rows(all_tokens, shared_gate_up)
    shared_part = jnp.dot(shared_hidden, shared_down, preferred_element_type=jnp.float32)
    shared_scale = jax.nn.sigmoid(
        jnp.dot(all_tokens, shared_gate, preferred_element_type=jnp.float32)
    )
    expert_out = kept + from_chip(sent, row_partner).astype(jnp.float32)
    routed = jnp.dot(pick, expert_out.astype(jnp.bfloat16), preferred_element_type=jnp.float32)
    share = shared_scale[:, None] * shared_part + factor * routed
    share = share.reshape(near, planes // near, tok_rows, width)
    return reduce_planes(share, near).astype(jnp.bfloat16)


def solution(mesh):
    in_specs = (
        P(("groups", "plane", "depth", "tok"), None),
        P(("groups", "plane", "depth", "tok"), None),
        P(("groups", "plane", "depth", "tok"), None),
        P(("groups", "plane", "depth", "tok"), None),
        P(),
        P(None, None, "plane"),
        P("plane", None),
        P("plane", None, None, ("depth", "tok")),
        P("plane", ("depth", "tok"), None),
    )
    out_specs = P(("groups", "plane", "depth", "tok"), None)
    return jax.shard_map(
        on_device, mesh=mesh, in_specs=in_specs, out_specs=out_specs, check_vma=False
    )
```

```python
import functools

import jax
import jax.numpy as jnp
from jax import lax
from jax.experimental import pallas as pl
from jax.experimental.pallas import tpu as pltpu
from jax.sharding import PartitionSpec as P

LANES = 128
KERNEL_VMEM = 14 << 20
GLUE_VMEM = 10 << 20


def from_offset(block, axis, offset):
    size, cores = lax.axis_size(axis), lax.axis_size("tok")
    pairs = [
        (((i + (-offset if t % 2 else offset)) % size) * cores + t, i * cores + t)
        for i in range(size)
        for t in range(cores)
    ]
    return lax.ppermute(block, (axis, "tok"), pairs)


def from_core(block):
    size = lax.axis_size("tok")
    return lax.ppermute(block, "tok", [((i + 1) % size, i) for i in range(size)])


def far_groups(planes, near):
    return [[r + near * f for f in range(planes // near)] for r in range(near)]


def gather_planes(block, near):
    groups = far_groups(lax.axis_size("plane"), near)
    own = lax.all_gather(block, "plane", axis_index_groups=groups, tiled=True)
    return [own] + [from_offset(own, "plane", k) for k in (1, 2, -1)]


def reduce_planes(own, sent, near, rows):
    total = own
    for block, k in zip(sent, (1, 2, -1)):
        total = total + from_offset(block, "plane", -k).astype(jnp.float32)
    arrived = lax.all_to_all(
        total.astype(jnp.bfloat16).reshape(-1, rows, total.shape[1]),
        "plane",
        split_axis=0,
        concat_axis=0,
        tiled=True,
        axis_index_groups=far_groups(lax.axis_size("plane"), near),
    )
    return arrived.astype(jnp.float32).sum(axis=0)


def from_chip(block, partner):
    size = lax.axis_size("depth")
    return lax.ppermute(block, "depth", [(partner(i, size), i) for i in range(size)])


def weight_partner(place, size):
    return place ^ 1


def row_partner(place, size):
    return size - 1 - place


def expert_kernel(own_ref, other_ref, *refs):
    shards = (len(refs) - 5) // 2
    gate_up_refs, down_refs = refs[:shards], refs[shards : 2 * shards]
    kept_ref, sent_ref, gate_up, down, sems = refs[2 * shards :]
    copies = []
    for s in range(shards):
        copies.append(pltpu.make_async_copy(gate_up_refs[s], gate_up.at[s], sems.at[2 * s]))
        copies.append(pltpu.make_async_copy(down_refs[s], down.at[s], sems.at[2 * s + 1]))
    for copy in copies:
        copy.start()
    rows = jnp.concatenate([own_ref[...], other_ref[...]])
    contract = (((1,), (1,)), ((), ()))
    total = None
    for s in range(shards):
        copies[2 * s].wait()
        gate = lax.dot_general(rows, gate_up[s, 0], contract, preferred_element_type=jnp.float32)
        up = lax.dot_general(rows, gate_up[s, 1], contract, preferred_element_type=jnp.float32)
        hidden = (gate / (1.0 + jnp.exp(-gate)) * up).astype(jnp.bfloat16)
        copies[2 * s + 1].wait()
        part = jnp.dot(hidden, down[s], preferred_element_type=jnp.float32)
        total = part if total is None else total + part
    half = own_ref.shape[0]
    kept_ref[...] = total[:half]
    sent_ref[...] = total[half:].astype(jnp.bfloat16)


def expert_partials(own, other, gate_ups, downs):
    rows, width = own.shape
    units = downs[0].shape[0]
    vmem, anywhere = pl.BlockSpec(memory_space=pltpu.VMEM), pl.BlockSpec(memory_space=pl.ANY)
    shards = len(downs)
    return pl.pallas_call(
        expert_kernel,
        out_shape=(
            jax.ShapeDtypeStruct((rows, width), jnp.float32),
            jax.ShapeDtypeStruct((rows, width), jnp.bfloat16),
        ),
        in_specs=[vmem, vmem] + [anywhere] * (2 * shards),
        out_specs=(vmem, vmem),
        scratch_shapes=[
            pltpu.VMEM((shards, 2, units, width), jnp.bfloat16),
            pltpu.VMEM((shards, units, width), jnp.bfloat16),
            pltpu.SemaphoreType.DMA((2 * shards,)),
        ],
        compiler_params=pltpu.CompilerParams(vmem_limit_bytes=KERNEL_VMEM),
        cost_estimate=pl.CostEstimate(
            flops=12 * shards * rows * width * units,
            bytes_accessed=6 * shards * units * width,
            transcendentals=2 * shards * rows * units,
        ),
    )(own, other, *gate_ups, *downs)


def notes_kernel(tokens_hbm, *refs, capacity):
    sources, out_ref, (ids_ref, slots_ref, weights_ref), sems = refs[:3], refs[3], refs[4:7], refs[7]
    width = tokens_hbm.shape[1]
    choices, rows = ids_ref.shape
    targets = (ids_ref, slots_ref, weights_ref)
    copies = [pltpu.make_async_copy(a, b, sems.at[i]) for i, (a, b) in enumerate(zip(sources, targets))]
    copies.append(pltpu.make_async_copy(tokens_hbm, out_ref.at[:, pl.ds(0, width)], sems.at[3]))
    for copy in copies:
        copy.start()
    for copy in copies[:3]:
        copy.wait()
    slots = slots_ref[...]
    code = jnp.where(slots < capacity, ids_ref[...] * capacity + slots, -1).astype(jnp.float32)
    notes = jnp.concatenate([code, weights_ref[...].astype(jnp.float32)])
    lane = lax.broadcasted_iota(jnp.int32, (rows, LANES), 1)
    row = lax.broadcasted_iota(jnp.int32, (rows, rows), 0)
    column = lax.broadcasted_iota(jnp.int32, (rows, rows), 1)
    placed = jnp.zeros((rows, LANES), jnp.float32)
    for k in range(2 * choices):
        spread = jnp.where(row == column, notes[k : k + 1, :], 0.0)
        value = jnp.sum(spread, axis=1, keepdims=True)
        placed = jnp.where(lane == k, value, placed)
    out_ref[:, width:] = placed.astype(jnp.bfloat16)
    copies[3].wait()


def picks_kernel(first_ref, *refs, capacity, choices, tok_rows):
    blocks, (rows_ref, mix_ref) = refs[:-2], refs[-2:]
    count, width = blocks[0].shape[0], rows_ref.shape[1]
    slots = mix_ref.shape[2]
    token = lax.broadcasted_iota(jnp.int32, (count, slots), 0)
    slot = lax.broadcasted_iota(jnp.int32, (count, slots), 1)
    wanted = (first_ref[0] + slot % capacity).astype(jnp.float32)
    here = slot // capacity == token // tok_rows
    for j, block in enumerate(blocks):
        notes = block[:, width:].astype(jnp.float32)
        weight = jnp.zeros((count, slots), jnp.float32)
        found = jnp.zeros((count, slots), jnp.float32)
        for k in range(choices):
            match = here & (notes[:, k : k + 1] == wanted)
            found = jnp.where(match, 1.0, found)
            weight = jnp.where(match, notes[:, choices + k : choices + k + 1], weight)
        rows = lax.dot_general(
            found.astype(jnp.bfloat16),
            block[:, :width],
            (((0,), (0,)), ((), ())),
            preferred_element_type=jnp.float32,
        )
        rows_ref[j * slots : (j + 1) * slots, :] = rows.astype(jnp.bfloat16)
        mix_ref[j] = weight.astype(jnp.bfloat16)


def shared_kernel(*refs):
    blocks, (gate_ref, gate_up_hbm, down_hbm, out_ref, gate_up, down, sems) = refs[:-7], refs[-7:]
    fetch_in = pltpu.make_async_copy(gate_up_hbm, gate_up, sems.at[0])
    fetch_out = pltpu.make_async_copy(down_hbm, down, sems.at[1])
    fetch_in.start()
    fetch_out.start()
    count, width = blocks[0].shape[0], out_ref.shape[2]
    gate_row = gate_ref[...].astype(jnp.float32)
    scales = []
    for block in blocks:
        score = jnp.sum(block[:, :width].astype(jnp.float32) * gate_row, axis=1, keepdims=True)
        scales.append(1.0 / (1.0 + jnp.exp(-score)))
    tokens = jnp.concatenate([block[:, :width] for block in blocks])
    contract = (((1,), (1,)), ((), ()))
    fetch_in.wait()
    gate = lax.dot_general(tokens, gate_up[0], contract, preferred_element_type=jnp.float32)
    up = lax.dot_general(tokens, gate_up[1], contract, preferred_element_type=jnp.float32)
    hidden = (gate / (1.0 + jnp.exp(-gate)) * up).astype(jnp.bfloat16)
    fetch_out.wait()
    for j, scale in enumerate(scales):
        part = hidden[j * count : (j + 1) * count]
        out_ref[j] = scale * jnp.dot(part, down[...], preferred_element_type=jnp.float32)


def combine_kernel(kept_ref, got_ref, mix_ref, shared_ref, own_ref, *sent_refs):
    rows = (kept_ref[...] + got_ref[...].astype(jnp.float32)).astype(jnp.bfloat16)
    slots = mix_ref.shape[2]
    for j, out_ref in enumerate((own_ref, *sent_refs)):
        part = rows[j * slots : (j + 1) * slots]
        routed = jnp.dot(mix_ref[j], part, preferred_element_type=jnp.float32)
        out_ref[...] = (shared_ref[j] + routed).astype(out_ref.dtype)


def in_vmem(count):
    return [pl.BlockSpec(memory_space=pltpu.VMEM)] * count


def on_device(
    tokens,
    expert_ids,
    slot_index,
    route_weight,
    shared_gate,
    shared_gate_up,
    shared_down,
    expert_gate_up,
    expert_down,
):
    planes = lax.axis_size("plane")
    tok_rows, width = tokens.shape
    choices = expert_ids.shape[1]
    capacity = max(2, tok_rows * choices // planes)
    near = 4
    count = planes // near * tok_rows
    slots = planes // near * capacity
    units = shared_down.shape[0]
    anywhere = pl.BlockSpec(memory_space=pl.ANY)
    small = pltpu.CompilerParams(vmem_limit_bytes=GLUE_VMEM)

    noted = pl.pallas_call(
        functools.partial(notes_kernel, capacity=capacity),
        out_shape=jax.ShapeDtypeStruct((tok_rows, width + LANES), jnp.bfloat16),
        in_specs=[pl.BlockSpec(memory_space=pltpu.HBM)] * 4,
        out_specs=in_vmem(1)[0],
        scratch_shapes=[
            pltpu.VMEM((choices, tok_rows), jnp.int32),
            pltpu.VMEM((choices, tok_rows), jnp.int32),
            pltpu.VMEM((choices, tok_rows), jnp.bfloat16),
            pltpu.SemaphoreType.DMA((4,)),
        ],
        compiler_params=pltpu.CompilerParams(vmem_limit_bytes=64 << 20),
    )(tokens, expert_ids.T, slot_index.T, route_weight.T)
    blocks = gather_planes(noted, near)

    first = (lax.axis_index("plane") * capacity).astype(jnp.int32).reshape(1)
    rows, mix = pl.pallas_call(
        functools.partial(
            picks_kernel, capacity=capacity, choices=choices, tok_rows=tok_rows
        ),
        out_shape=(
            jax.ShapeDtypeStruct((near * slots, width), jnp.bfloat16),
            jax.ShapeDtypeStruct((near, count, slots), jnp.bfloat16),
        ),
        in_specs=[pl.BlockSpec(memory_space=pltpu.SMEM)] + in_vmem(near),
        out_specs=tuple(in_vmem(2)),
        compiler_params=small,
    )(first, *blocks)

    gate_up, down = expert_gate_up[0].swapaxes(1, 2), expert_down[0]
    gate_up_chip = from_chip(gate_up, weight_partner)
    down_chip = from_chip(down, weight_partner)
    gate_up_core, down_core = from_core(gate_up), from_core(down)
    gate_up_far = from_core(gate_up_chip)
    down_far = from_core(down_chip)
    other_rows = from_chip(rows, row_partner)
    kept, sent = expert_partials(
        rows,
        other_rows,
        (gate_up, gate_up_core, gate_up_chip, gate_up_far),
        (down, down_core, down_chip, down_far),
    )
    got = from_chip(sent, row_partner)

    shared_part = pl.pallas_call(
        shared_kernel,
        out_shape=jax.ShapeDtypeStruct((near, count, width), jnp.float32),
        in_specs=in_vmem(near + 1) + [anywhere] * 2,
        out_specs=in_vmem(1)[0],
        scratch_shapes=[
            pltpu.VMEM((2, units, width), jnp.bfloat16),
            pltpu.VMEM((units, width), jnp.bfloat16),
            pltpu.SemaphoreType.DMA((2,)),
        ],
        compiler_params=pltpu.CompilerParams(vmem_limit_bytes=KERNEL_VMEM),
        cost_estimate=pl.CostEstimate(
            flops=6 * near * count * width * units,
            bytes_accessed=6 * units * width,
            transcendentals=near * count * units,
        ),
    )(*blocks, shared_gate.reshape(1, width), shared_gate_up.swapaxes(1, 2), shared_down)

    own, *others = pl.pallas_call(
        combine_kernel,
        out_shape=[jax.ShapeDtypeStruct((count, width), jnp.float32)]
        + [jax.ShapeDtypeStruct((count, width), jnp.bfloat16)] * (near - 1),
        in_specs=in_vmem(4),
        out_specs=in_vmem(near),
        compiler_params=small,
    )(kept, got, mix, shared_part)
    return reduce_planes(own, others, near, tok_rows).astype(jnp.bfloat16)


def solution(mesh):
    in_specs = (
        P(("groups", "plane", "depth", "tok"), None),
        P(("groups", "plane", "depth", "tok"), None),
        P(("groups", "plane", "depth", "tok"), None),
        P(("groups", "plane", "depth", "tok"), None),
        P(),
        P(None, None, "plane"),
        P("plane", None),
        P("plane", None, None, ("depth", "tok")),
        P("plane", ("depth", "tok"), None),
    )
    out_specs = P(("groups", "plane", "depth", "tok"), None)
    return jax.shard_map(on_device, mesh=mesh, in_specs=in_specs, out_specs=out_specs, check_vma=False)
```

```python
import functools

import jax
import jax.numpy as jnp
from jax import lax
from jax.experimental import pallas as pl
from jax.experimental.pallas import tpu as pltpu
from jax.sharding import PartitionSpec as P

LANES = 128
KERNEL_VMEM = 14 << 20
GLUE_VMEM = 10 << 20


def from_offset(block, axis, offset):
    size, cores = lax.axis_size(axis), lax.axis_size("tok")
    pairs = [
        (((i + (-offset if t % 2 else offset)) % size) * cores + t, i * cores + t)
        for i in range(size)
        for t in range(cores)
    ]
    return lax.ppermute(block, (axis, "tok"), pairs)


def from_core(block):
    size = lax.axis_size("tok")
    return lax.ppermute(block, "tok", [((i + 1) % size, i) for i in range(size)])


def far_groups(planes, near):
    return [[r + near * f for f in range(planes // near)] for r in range(near)]


def gather_planes(block, near):
    groups = far_groups(lax.axis_size("plane"), near)
    own = lax.all_gather(block, "plane", axis_index_groups=groups, tiled=True)
    return [own] + [from_offset(own, "plane", k) for k in (1, 2, -1)]


def reduce_planes(own, sent, near, rows):
    total = own
    for block, k in zip(sent, (1, 2, -1)):
        arrived = from_offset(block, "plane", -k)
        total = total + arrived.astype(jnp.float32)
    arrived = lax.all_to_all(
        total.astype(jnp.bfloat16).reshape(-1, rows, total.shape[1]),
        "plane",
        split_axis=0,
        concat_axis=0,
        tiled=True,
        axis_index_groups=far_groups(lax.axis_size("plane"), near),
    )
    return arrived.astype(jnp.float32).sum(axis=0)


def from_chip(block, partner):
    size = lax.axis_size("depth")
    return lax.ppermute(block, "depth", [(partner(i, size), i) for i in range(size)])


def weight_partner(place, size):
    return place ^ 1


def row_partner(place, size):
    return size - 1 - place


def expert_kernel(own_ref, other_ref, *refs):
    shards = (len(refs) - 5) // 2
    gate_up_refs, down_refs = refs[:shards], refs[shards : 2 * shards]
    kept_ref, sent_ref, gate_up, down, sems = refs[2 * shards :]
    fetch_in = pltpu.make_async_copy(gate_up_refs[-1], gate_up, sems.at[0])
    fetch_out = pltpu.make_async_copy(down_refs[-1], down, sems.at[1])
    fetch_in.start()
    fetch_out.start()
    rows = jnp.concatenate([own_ref[...], other_ref[...]])
    contract = (((1,), (1,)), ((), ()))
    total = None
    for s in range(shards):
        last = s == shards - 1
        if last:
            fetch_in.wait()
        both = gate_up if last else gate_up_refs[s]
        gate = lax.dot_general(rows, both[0], contract, preferred_element_type=jnp.float32)
        up = lax.dot_general(rows, both[1], contract, preferred_element_type=jnp.float32)
        hidden = (gate / (1.0 + jnp.exp(-gate)) * up).astype(jnp.bfloat16)
        if last:
            fetch_out.wait()
        weights = down if last else down_refs[s]
        part = jnp.dot(hidden, weights[...], preferred_element_type=jnp.float32)
        total = part if total is None else total + part
    half = own_ref.shape[0]
    kept_ref[...] = total[:half]
    sent_ref[...] = total[half:].astype(jnp.bfloat16)


def expert_partials(own, other, gate_ups, downs):
    rows, width = own.shape
    units = downs[0].shape[0]
    shards = len(downs)
    anywhere = pl.BlockSpec(memory_space=pl.ANY)
    weights = in_vmem(shards - 1) + [anywhere]
    return pl.pallas_call(
        expert_kernel,
        out_shape=(
            jax.ShapeDtypeStruct((rows, width), jnp.float32),
            jax.ShapeDtypeStruct((rows, width), jnp.bfloat16),
        ),
        in_specs=in_vmem(2) + weights * 2,
        out_specs=tuple(in_vmem(2)),
        scratch_shapes=[
            pltpu.VMEM((2, units, width), jnp.bfloat16),
            pltpu.VMEM((units, width), jnp.bfloat16),
            pltpu.SemaphoreType.DMA((2,)),
        ],
        compiler_params=pltpu.CompilerParams(vmem_limit_bytes=KERNEL_VMEM),
        cost_estimate=pl.CostEstimate(
            flops=12 * shards * rows * width * units,
            bytes_accessed=6 * shards * units * width,
            transcendentals=2 * shards * rows * units,
        ),
    )(own, other, *gate_ups, *downs)


def notes_kernel(tokens_hbm, *refs, capacity):
    sources, out_ref, (ids_ref, slots_ref, weights_ref), sems = refs[:3], refs[3], refs[4:7], refs[7]
    width = tokens_hbm.shape[1]
    choices, rows = ids_ref.shape
    targets = (ids_ref, slots_ref, weights_ref)
    copies = [pltpu.make_async_copy(a, b, sems.at[i]) for i, (a, b) in enumerate(zip(sources, targets))]
    copies.append(pltpu.make_async_copy(tokens_hbm, out_ref.at[:, pl.ds(0, width)], sems.at[3]))
    for copy in copies:
        copy.start()
    for copy in copies[:3]:
        copy.wait()
    slots = slots_ref[...]
    code = jnp.where(slots < capacity, ids_ref[...] * capacity + slots, -1).astype(jnp.float32)
    notes = jnp.concatenate([code, weights_ref[...].astype(jnp.float32)])
    lane = lax.broadcasted_iota(jnp.int32, (rows, LANES), 1)
    row = lax.broadcasted_iota(jnp.int32, (rows, rows), 0)
    column = lax.broadcasted_iota(jnp.int32, (rows, rows), 1)
    placed = jnp.zeros((rows, LANES), jnp.float32)
    for k in range(2 * choices):
        spread = jnp.where(row == column, notes[k : k + 1, :], 0.0)
        value = jnp.sum(spread, axis=1, keepdims=True)
        placed = jnp.where(lane == k, value, placed)
    out_ref[:, width:] = placed.astype(jnp.bfloat16)
    copies[3].wait()


def picks_kernel(first_ref, *refs, capacity, choices, tok_rows):
    blocks, (rows_ref, mix_ref) = refs[:-2], refs[-2:]
    count, width = blocks[0].shape[0], rows_ref.shape[1]
    slots = mix_ref.shape[2]
    token = lax.broadcasted_iota(jnp.int32, (count, slots), 0)
    slot = lax.broadcasted_iota(jnp.int32, (count, slots), 1)
    wanted = (first_ref[0] + slot % capacity).astype(jnp.float32)
    here = slot // capacity == token // tok_rows
    for j, block in enumerate(blocks):
        notes = block[:, width:].astype(jnp.float32)
        weight = jnp.zeros((count, slots), jnp.float32)
        found = jnp.zeros((count, slots), jnp.float32)
        for k in range(choices):
            match = here & (notes[:, k : k + 1] == wanted)
            found = jnp.where(match, 1.0, found)
            weight = jnp.where(match, notes[:, choices + k : choices + k + 1], weight)
        rows = lax.dot_general(
            found.astype(jnp.bfloat16),
            block[:, :width],
            (((0,), (0,)), ((), ())),
            preferred_element_type=jnp.float32,
        )
        rows_ref[j * slots : (j + 1) * slots, :] = rows.astype(jnp.bfloat16)
        mix_ref[j] = weight.astype(jnp.bfloat16)


def shared_kernel(*refs):
    blocks, (gate_ref, gate_up_hbm, down_hbm, out_ref, gate_up, down, sems) = refs[:-7], refs[-7:]
    fetch_in = pltpu.make_async_copy(gate_up_hbm, gate_up, sems.at[0])
    fetch_out = pltpu.make_async_copy(down_hbm, down, sems.at[1])
    fetch_in.start()
    fetch_out.start()
    count, width = blocks[0].shape[0], out_ref.shape[2]
    gate_row = gate_ref[...].astype(jnp.float32)
    scales = []
    for block in blocks:
        score = jnp.sum(block[:, :width].astype(jnp.float32) * gate_row, axis=1, keepdims=True)
        scales.append(1.0 / (1.0 + jnp.exp(-score)))
    tokens = jnp.concatenate([block[:, :width] for block in blocks])
    contract = (((1,), (1,)), ((), ()))
    fetch_in.wait()
    gate = lax.dot_general(tokens, gate_up[0], contract, preferred_element_type=jnp.float32)
    up = lax.dot_general(tokens, gate_up[1], contract, preferred_element_type=jnp.float32)
    hidden = (gate / (1.0 + jnp.exp(-gate)) * up).astype(jnp.bfloat16)
    fetch_out.wait()
    for j, scale in enumerate(scales):
        part = hidden[j * count : (j + 1) * count]
        out_ref[j] = scale * jnp.dot(part, down[...], preferred_element_type=jnp.float32)


def combine_kernel(kept_ref, got_ref, mix_ref, shared_ref, own_ref, *sent_refs):
    rows = (kept_ref[...] + got_ref[...].astype(jnp.float32)).astype(jnp.bfloat16)
    slots = mix_ref.shape[2]
    for j, out_ref in enumerate((own_ref, *sent_refs)):
        part = rows[j * slots : (j + 1) * slots]
        routed = jnp.dot(mix_ref[j], part, preferred_element_type=jnp.float32)
        out_ref[...] = (shared_ref[j] + routed).astype(out_ref.dtype)


def in_vmem(count):
    return [pl.BlockSpec(memory_space=pltpu.VMEM)] * count


def on_device(
    tokens,
    expert_ids,
    slot_index,
    route_weight,
    shared_gate,
    shared_gate_up,
    shared_down,
    expert_gate_up,
    expert_down,
):
    planes = lax.axis_size("plane")
    tok_rows, width = tokens.shape
    choices = expert_ids.shape[1]
    capacity = max(2, tok_rows * choices // planes)
    near = 4
    count = planes // near * tok_rows
    slots = planes // near * capacity
    units = shared_down.shape[0]
    anywhere = pl.BlockSpec(memory_space=pl.ANY)
    small = pltpu.CompilerParams(vmem_limit_bytes=GLUE_VMEM)

    noted = pl.pallas_call(
        functools.partial(notes_kernel, capacity=capacity),
        out_shape=jax.ShapeDtypeStruct((tok_rows, width + LANES), jnp.bfloat16),
        in_specs=[pl.BlockSpec(memory_space=pltpu.HBM)] * 4,
        out_specs=in_vmem(1)[0],
        scratch_shapes=[
            pltpu.VMEM((choices, tok_rows), jnp.int32),
            pltpu.VMEM((choices, tok_rows), jnp.int32),
            pltpu.VMEM((choices, tok_rows), jnp.bfloat16),
            pltpu.SemaphoreType.DMA((4,)),
        ],
        compiler_params=pltpu.CompilerParams(vmem_limit_bytes=64 << 20),
    )(tokens, expert_ids.T, slot_index.T, route_weight.T)
    blocks = gather_planes(noted, near)

    first = (lax.axis_index("plane") * capacity).astype(jnp.int32).reshape(1)
    rows, mix = pl.pallas_call(
        functools.partial(
            picks_kernel, capacity=capacity, choices=choices, tok_rows=tok_rows
        ),
        out_shape=(
            jax.ShapeDtypeStruct((near * slots, width), jnp.bfloat16),
            jax.ShapeDtypeStruct((near, count, slots), jnp.bfloat16),
        ),
        in_specs=[pl.BlockSpec(memory_space=pltpu.SMEM)] + in_vmem(near),
        out_specs=tuple(in_vmem(2)),
        compiler_params=small,
    )(first, *blocks)

    gate_up, down = expert_gate_up[0].swapaxes(1, 2), expert_down[0]
    gate_up_chip = from_chip(gate_up, weight_partner)
    down_chip = from_chip(down, weight_partner)
    gate_up_core, down_core = from_core(gate_up), from_core(down)
    gate_up_far = from_core(gate_up_chip)
    down_far = from_core(down_chip)
    other_rows = from_chip(rows, row_partner)
    kept, sent = expert_partials(
        rows,
        other_rows,
        (gate_up, gate_up_core, gate_up_far, gate_up_chip),
        (down, down_core, down_far, down_chip),
    )
    got = from_chip(sent, row_partner)

    shared_part = pl.pallas_call(
        shared_kernel,
        out_shape=jax.ShapeDtypeStruct((near, count, width), jnp.float32),
        in_specs=in_vmem(near + 1) + [anywhere] * 2,
        out_specs=in_vmem(1)[0],
        scratch_shapes=[
            pltpu.VMEM((2, units, width), jnp.bfloat16),
            pltpu.VMEM((units, width), jnp.bfloat16),
            pltpu.SemaphoreType.DMA((2,)),
        ],
        compiler_params=pltpu.CompilerParams(vmem_limit_bytes=KERNEL_VMEM),
        cost_estimate=pl.CostEstimate(
            flops=6 * near * count * width * units,
            bytes_accessed=6 * units * width,
            transcendentals=near * count * units,
        ),
    )(*blocks, shared_gate.reshape(1, width), shared_gate_up.swapaxes(1, 2), shared_down)

    own, *others = pl.pallas_call(
        combine_kernel,
        out_shape=[jax.ShapeDtypeStruct((count, width), jnp.float32)]
        + [jax.ShapeDtypeStruct((count, width), jnp.bfloat16)] * (near - 1),
        in_specs=in_vmem(4),
        out_specs=in_vmem(near),
        compiler_params=small,
    )(kept, got, mix, shared_part)
    return reduce_planes(own, others, near, tok_rows).astype(jnp.bfloat16)


def solution(mesh):
    in_specs = (
        P(("groups", "plane", "depth", "tok"), None),
        P(("groups", "plane", "depth", "tok"), None),
        P(("groups", "plane", "depth", "tok"), None),
        P(("groups", "plane", "depth", "tok"), None),
        P(),
        P(None, None, "plane"),
        P("plane", None),
        P("plane", None, None, ("depth", "tok")),
        P("plane", ("depth", "tok"), None),
    )
    out_specs = P(("groups", "plane", "depth", "tok"), None)
    return jax.shard_map(on_device, mesh=mesh, in_specs=in_specs, out_specs=out_specs, check_vma=False)
```

```python
import functools

import jax
import jax.numpy as jnp
from jax import lax
from jax.experimental import pallas as pl
from jax.experimental.pallas import tpu as pltpu
from jax.sharding import PartitionSpec as P

LANES = 128
KERNEL_VMEM = 14 << 20
GLUE_VMEM = 10 << 20


def from_offset(block, axis, offset):
    size, cores = lax.axis_size(axis), lax.axis_size("tok")
    pairs = [
        (((i + (-offset if t % 2 else offset)) % size) * cores + t, i * cores + t)
        for i in range(size)
        for t in range(cores)
    ]
    return lax.ppermute(block, (axis, "tok"), pairs)


def from_core(block):
    size = lax.axis_size("tok")
    return lax.ppermute(block, "tok", [((i + 1) % size, i) for i in range(size)])


def far_groups(planes, near):
    return [[r + near * f for f in range(planes // near)] for r in range(near)]


def gather_planes(block, near):
    groups = far_groups(lax.axis_size("plane"), near)
    own = lax.all_gather(block, "plane", axis_index_groups=groups, tiled=True)
    return [own] + [from_offset(own, "plane", k) for k in (1, 2, -1)]


def reduce_planes(own, sent, near, rows):
    total = own
    for block, k in zip(sent, (1, 2, -1)):
        arrived = from_offset(block, "plane", -k)
        total = total + arrived.astype(jnp.float32)
    arrived = lax.all_to_all(
        total.astype(jnp.bfloat16).reshape(-1, rows, total.shape[1]),
        "plane",
        split_axis=0,
        concat_axis=0,
        tiled=True,
        axis_index_groups=far_groups(lax.axis_size("plane"), near),
    )
    return arrived.astype(jnp.float32).sum(axis=0)


def from_chip(block, partner):
    size = lax.axis_size("depth")
    return lax.ppermute(block, "depth", [(partner(i, size), i) for i in range(size)])


def weight_partner(place, size):
    return place ^ 1


def row_partner(place, size):
    return size - 1 - place


def expert_kernel(own_ref, other_ref, *refs):
    shards = (len(refs) - 5) // 2
    gate_up_refs, down_refs = refs[:shards], refs[shards : 2 * shards]
    kept_ref, sent_ref, gate_up, down, sems = refs[2 * shards :]
    fetch_in = pltpu.make_async_copy(gate_up_refs[-1], gate_up, sems.at[0])
    fetch_out = pltpu.make_async_copy(down_refs[-1], down, sems.at[1])
    fetch_in.start()
    fetch_out.start()
    rows = jnp.concatenate([own_ref[...], other_ref[...]])
    contract = (((1,), (1,)), ((), ()))
    total = None
    for s in range(shards):
        last = s == shards - 1
        if last:
            fetch_in.wait()
        both = gate_up if last else gate_up_refs[s]
        gate = lax.dot_general(rows, both[0], contract, preferred_element_type=jnp.float32)
        up = lax.dot_general(rows, both[1], contract, preferred_element_type=jnp.float32)
        hidden = (gate / (1.0 + jnp.exp(-gate)) * up).astype(jnp.bfloat16)
        if last:
            fetch_out.wait()
        weights = down if last else down_refs[s]
        part = jnp.dot(hidden, weights[...], preferred_element_type=jnp.float32)
        total = part if total is None else total + part
    half = own_ref.shape[0]
    kept_ref[...] = total[:half]
    sent_ref[...] = total[half:].astype(jnp.bfloat16)


def expert_partials(own, other, gate_ups, downs):
    rows, width = own.shape
    units = downs[0].shape[0]
    shards = len(downs)
    anywhere = pl.BlockSpec(memory_space=pl.ANY)
    weights = in_vmem(shards - 1) + [anywhere]
    return pl.pallas_call(
        expert_kernel,
        out_shape=(
            jax.ShapeDtypeStruct((rows, width), jnp.float32),
            jax.ShapeDtypeStruct((rows, width), jnp.bfloat16),
        ),
        in_specs=in_vmem(2) + weights * 2,
        out_specs=tuple(in_vmem(2)),
        scratch_shapes=[
            pltpu.VMEM((2, units, width), jnp.bfloat16),
            pltpu.VMEM((units, width), jnp.bfloat16),
            pltpu.SemaphoreType.DMA((2,)),
        ],
        compiler_params=pltpu.CompilerParams(vmem_limit_bytes=KERNEL_VMEM),
        cost_estimate=pl.CostEstimate(
            flops=12 * shards * rows * width * units,
            bytes_accessed=6 * shards * units * width,
            transcendentals=2 * shards * rows * units,
        ),
    )(own, other, *gate_ups, *downs)


def notes_kernel(tokens_hbm, *refs):
    sources, out_ref, (ids_ref, slots_ref, weights_ref), sems = refs[:3], refs[3], refs[4:7], refs[7]
    width = tokens_hbm.shape[1]
    choices, rows = ids_ref.shape
    targets = (ids_ref, slots_ref, weights_ref)
    copies = [pltpu.make_async_copy(a, b, sems.at[i]) for i, (a, b) in enumerate(zip(sources, targets))]
    copies.append(pltpu.make_async_copy(tokens_hbm, out_ref.at[:, pl.ds(0, width)], sems.at[3]))
    for copy in copies:
        copy.start()
    for copy in copies[:3]:
        copy.wait()
    notes = jnp.concatenate([ref[...].astype(jnp.float32) for ref in targets])
    lane = lax.broadcasted_iota(jnp.int32, (rows, LANES), 1)
    row = lax.broadcasted_iota(jnp.int32, (rows, rows), 0)
    column = lax.broadcasted_iota(jnp.int32, (rows, rows), 1)
    placed = jnp.zeros((rows, LANES), jnp.float32)
    for k in range(3 * choices):
        spread = jnp.where(row == column, notes[k : k + 1, :], 0.0)
        value = jnp.sum(spread, axis=1, keepdims=True)
        placed = jnp.where(lane == k, value, placed)
    out_ref[:, width:] = placed.astype(jnp.bfloat16)
    copies[3].wait()


def picks_kernel(expert_ref, *refs, capacity, choices, tok_rows):
    blocks, (rows_ref, mix_ref) = refs[:-2], refs[-2:]
    count, width = blocks[0].shape[0], rows_ref.shape[1]
    slots = mix_ref.shape[2]
    token = lax.broadcasted_iota(jnp.int32, (count, slots), 0)
    slot = lax.broadcasted_iota(jnp.int32, (count, slots), 1)
    mine = expert_ref[0].astype(jnp.float32)
    wanted = (slot % capacity).astype(jnp.float32)
    here = slot // capacity == token // tok_rows
    for j, block in enumerate(blocks):
        notes = block[:, width:].astype(jnp.float32)
        weight = jnp.zeros((count, slots), jnp.float32)
        found = jnp.zeros((count, slots), jnp.float32)
        for k in range(choices):
            expert = notes[:, k : k + 1]
            place = notes[:, choices + k : choices + k + 1]
            value = notes[:, 2 * choices + k : 2 * choices + k + 1]
            match = here & (expert == mine) & (place == wanted)
            found = jnp.where(match, 1.0, found)
            weight = jnp.where(match, value, weight)
        rows = lax.dot_general(
            found.astype(jnp.bfloat16),
            block[:, :width],
            (((0,), (0,)), ((), ())),
            preferred_element_type=jnp.float32,
        )
        rows_ref[j * slots : (j + 1) * slots, :] = rows.astype(jnp.bfloat16)
        mix_ref[j] = weight.astype(jnp.bfloat16)


def shared_kernel(*refs):
    blocks, (gate_ref, gate_up_hbm, down_hbm, out_ref, gate_up, down, sems) = refs[:-7], refs[-7:]
    fetch_in = pltpu.make_async_copy(gate_up_hbm, gate_up, sems.at[0])
    fetch_out = pltpu.make_async_copy(down_hbm, down, sems.at[1])
    fetch_in.start()
    fetch_out.start()
    count, width = blocks[0].shape[0], out_ref.shape[2]
    gate_row = gate_ref[...].astype(jnp.float32)
    scales = []
    for block in blocks:
        score = jnp.sum(block[:, :width].astype(jnp.float32) * gate_row, axis=1, keepdims=True)
        scales.append(1.0 / (1.0 + jnp.exp(-score)))
    tokens = jnp.concatenate([block[:, :width] for block in blocks])
    contract = (((1,), (1,)), ((), ()))
    fetch_in.wait()
    gate = lax.dot_general(tokens, gate_up[0], contract, preferred_element_type=jnp.float32)
    up = lax.dot_general(tokens, gate_up[1], contract, preferred_element_type=jnp.float32)
    hidden = (gate / (1.0 + jnp.exp(-gate)) * up).astype(jnp.bfloat16)
    fetch_out.wait()
    for j, scale in enumerate(scales):
        part = hidden[j * count : (j + 1) * count]
        out_ref[j] = scale * jnp.dot(part, down[...], preferred_element_type=jnp.float32)


def combine_kernel(kept_ref, got_ref, mix_ref, shared_ref, own_ref, *sent_refs):
    rows = (kept_ref[...] + got_ref[...].astype(jnp.float32)).astype(jnp.bfloat16)
    slots = mix_ref.shape[2]
    for j, out_ref in enumerate((own_ref, *sent_refs)):
        part = rows[j * slots : (j + 1) * slots]
        routed = jnp.dot(mix_ref[j], part, preferred_element_type=jnp.float32)
        out_ref[...] = (shared_ref[j] + routed).astype(out_ref.dtype)


def in_vmem(count):
    return [pl.BlockSpec(memory_space=pltpu.VMEM)] * count


def on_device(
    tokens,
    expert_ids,
    slot_index,
    route_weight,
    shared_gate,
    shared_gate_up,
    shared_down,
    expert_gate_up,
    expert_down,
):
    planes = lax.axis_size("plane")
    tok_rows, width = tokens.shape
    choices = expert_ids.shape[1]
    capacity = max(2, tok_rows * choices // planes)
    near = 4
    count = planes // near * tok_rows
    slots = planes // near * capacity
    units = shared_down.shape[0]
    anywhere = pl.BlockSpec(memory_space=pl.ANY)
    small = pltpu.CompilerParams(vmem_limit_bytes=GLUE_VMEM)

    noted = pl.pallas_call(
        notes_kernel,
        out_shape=jax.ShapeDtypeStruct((tok_rows, width + LANES), jnp.bfloat16),
        in_specs=[pl.BlockSpec(memory_space=pltpu.HBM)] * 4,
        out_specs=in_vmem(1)[0],
        scratch_shapes=[
            pltpu.VMEM((choices, tok_rows), jnp.int32),
            pltpu.VMEM((choices, tok_rows), jnp.int32),
            pltpu.VMEM((choices, tok_rows), jnp.bfloat16),
            pltpu.SemaphoreType.DMA((4,)),
        ],
        compiler_params=pltpu.CompilerParams(vmem_limit_bytes=64 << 20),
    )(tokens, expert_ids.T, slot_index.T, route_weight.T)
    blocks = gather_planes(noted, near)

    expert = lax.axis_index("plane").astype(jnp.int32).reshape(1)
    rows, mix = pl.pallas_call(
        functools.partial(
            picks_kernel, capacity=capacity, choices=choices, tok_rows=tok_rows
        ),
        out_shape=(
            jax.ShapeDtypeStruct((near * slots, width), jnp.bfloat16),
            jax.ShapeDtypeStruct((near, count, slots), jnp.bfloat16),
        ),
        in_specs=[pl.BlockSpec(memory_space=pltpu.SMEM)] + in_vmem(near),
        out_specs=tuple(in_vmem(2)),
        compiler_params=small,
    )(expert, *blocks)

    gate_up, down = expert_gate_up[0].swapaxes(1, 2), expert_down[0]
    gate_up_chip = from_chip(gate_up, weight_partner)
    down_chip = from_chip(down, weight_partner)
    gate_up_core, down_core = from_core(gate_up), from_core(down)
    gate_up_far = from_core(gate_up_chip)
    down_far = from_core(down_chip)
    other_rows = from_chip(rows, row_partner)
    kept, sent = expert_partials(
        rows,
        other_rows,
        (gate_up, gate_up_core, gate_up_far, gate_up_chip),
        (down, down_core, down_far, down_chip),
    )
    got = from_chip(sent, row_partner)

    shared_part = pl.pallas_call(
        shared_kernel,
        out_shape=jax.ShapeDtypeStruct((near, count, width), jnp.float32),
        in_specs=in_vmem(near + 1) + [anywhere] * 2,
        out_specs=in_vmem(1)[0],
        scratch_shapes=[
            pltpu.VMEM((2, units, width), jnp.bfloat16),
            pltpu.VMEM((units, width), jnp.bfloat16),
            pltpu.SemaphoreType.DMA((2,)),
        ],
        compiler_params=pltpu.CompilerParams(vmem_limit_bytes=KERNEL_VMEM),
        cost_estimate=pl.CostEstimate(
            flops=6 * near * count * width * units,
            bytes_accessed=6 * units * width,
            transcendentals=near * count * units,
        ),
    )(*blocks, shared_gate.reshape(1, width), shared_gate_up.swapaxes(1, 2), shared_down)

    own, *others = pl.pallas_call(
        combine_kernel,
        out_shape=[jax.ShapeDtypeStruct((count, width), jnp.float32)]
        + [jax.ShapeDtypeStruct((count, width), jnp.bfloat16)] * (near - 1),
        in_specs=in_vmem(4),
        out_specs=in_vmem(near),
        compiler_params=small,
    )(kept, got, mix, shared_part)
    return reduce_planes(own, others, near, tok_rows).astype(jnp.bfloat16)


def solution(mesh):
    in_specs = (
        P(("groups", "plane", "depth", "tok"), None),
        P(("groups", "plane", "depth", "tok"), None),
        P(("groups", "plane", "depth", "tok"), None),
        P(("groups", "plane", "depth", "tok"), None),
        P(),
        P(None, None, "plane"),
        P("plane", None),
        P("plane", None, None, ("depth", "tok")),
        P("plane", ("depth", "tok"), None),
    )
    out_specs = P(("groups", "plane", "depth", "tok"), None)
    return jax.shard_map(on_device, mesh=mesh, in_specs=in_specs, out_specs=out_specs, check_vma=False)
```

```python
import functools

import jax
import jax.numpy as jnp
from jax import lax
from jax.experimental import pallas as pl
from jax.experimental.pallas import tpu as pltpu
from jax.sharding import PartitionSpec as P

LANES = 128
KERNEL_VMEM = 14 << 20
GLUE_VMEM = 10 << 20


def from_offset(block, axis, offset):
    size, cores = lax.axis_size(axis), lax.axis_size("tok")
    pairs = [
        (((i + (-offset if t % 2 else offset)) % size) * cores + t, i * cores + t)
        for i in range(size)
        for t in range(cores)
    ]
    return lax.ppermute(block, (axis, "tok"), pairs)


def from_core(block):
    size = lax.axis_size("tok")
    return lax.ppermute(block, "tok", [((i + 1) % size, i) for i in range(size)])


def far_groups(planes, near):
    return [[r + near * f for f in range(planes // near)] for r in range(near)]


def gather_planes(block, near):
    groups = far_groups(lax.axis_size("plane"), near)
    own = lax.all_gather(block, "plane", axis_index_groups=groups, tiled=True)
    return [own] + [from_offset(own, "plane", k) for k in (1, 2, -1)]


def reduce_planes(own, sent, near, rows):
    total = own
    for block, k in zip(sent, (1, 2, -1)):
        arrived = from_offset(block, "plane", -k)
        total = total + arrived.astype(jnp.float32)
    arrived = lax.all_to_all(
        total.astype(jnp.bfloat16).reshape(-1, rows, total.shape[1]),
        "plane",
        split_axis=0,
        concat_axis=0,
        tiled=True,
        axis_index_groups=far_groups(lax.axis_size("plane"), near),
    )
    return arrived.astype(jnp.float32).sum(axis=0)


def from_chip(block, partner):
    size = lax.axis_size("depth")
    return lax.ppermute(block, "depth", [(partner(i, size), i) for i in range(size)])


def weight_partner(place, size):
    return place ^ 1


def row_partner(place, size):
    return size - 1 - place


def expert_kernel(own_ref, other_ref, *refs):
    shards = (len(refs) - 5) // 2
    gate_up_refs, down_refs = refs[:shards], refs[shards : 2 * shards]
    kept_ref, sent_ref, gate_up, down, sems = refs[2 * shards :]
    fetch_in = pltpu.make_async_copy(gate_up_refs[-1], gate_up, sems.at[0])
    fetch_out = pltpu.make_async_copy(down_refs[-1], down, sems.at[1])
    fetch_in.start()
    fetch_out.start()
    rows = jnp.concatenate([own_ref[...], other_ref[...]])
    contract = (((1,), (1,)), ((), ()))
    total = None
    for s in range(shards):
        last = s == shards - 1
        if last:
            fetch_in.wait()
        both = gate_up if last else gate_up_refs[s]
        gate = lax.dot_general(rows, both[0], contract, preferred_element_type=jnp.float32)
        up = lax.dot_general(rows, both[1], contract, preferred_element_type=jnp.float32)
        hidden = (gate / (1.0 + jnp.exp(-gate)) * up).astype(jnp.bfloat16)
        if last:
            fetch_out.wait()
        weights = down if last else down_refs[s]
        part = jnp.dot(hidden, weights[...], preferred_element_type=jnp.float32)
        total = part if total is None else total + part
    half = own_ref.shape[0]
    kept_ref[...] = total[:half]
    sent_ref[...] = total[half:].astype(jnp.bfloat16)


def expert_partials(own, other, gate_ups, downs):
    rows, width = own.shape
    units = downs[0].shape[0]
    shards = len(downs)
    anywhere = pl.BlockSpec(memory_space=pl.ANY)
    weights = in_vmem(shards - 1) + [anywhere]
    return pl.pallas_call(
        expert_kernel,
        out_shape=(
            jax.ShapeDtypeStruct((rows, width), jnp.float32),
            jax.ShapeDtypeStruct((rows, width), jnp.bfloat16),
        ),
        in_specs=in_vmem(2) + weights * 2,
        out_specs=tuple(in_vmem(2)),
        scratch_shapes=[
            pltpu.VMEM((2, units, width), jnp.bfloat16),
            pltpu.VMEM((units, width), jnp.bfloat16),
            pltpu.SemaphoreType.DMA((2,)),
        ],
        compiler_params=pltpu.CompilerParams(vmem_limit_bytes=KERNEL_VMEM),
        cost_estimate=pl.CostEstimate(
            flops=12 * shards * rows * width * units,
            bytes_accessed=6 * shards * units * width,
            transcendentals=2 * shards * rows * units,
        ),
    )(own, other, *gate_ups, *downs)


def notes_kernel(tokens_hbm, *refs):
    sources, out_ref, (ids_ref, slots_ref, weights_ref), sems = refs[:3], refs[3], refs[4:7], refs[7]
    width = tokens_hbm.shape[1]
    choices = ids_ref.shape[0]
    targets = (ids_ref, slots_ref, weights_ref)
    copies = [pltpu.make_async_copy(a, b, sems.at[i]) for i, (a, b) in enumerate(zip(sources, targets))]
    copies.append(pltpu.make_async_copy(tokens_hbm, out_ref.at[:, pl.ds(0, width)], sems.at[3]))
    for copy in copies:
        copy.start()
    for copy in copies[:3]:
        copy.wait()
    notes = jnp.concatenate([ref[...].astype(jnp.float32) for ref in targets])
    kind = lax.broadcasted_iota(jnp.int32, (3 * choices, LANES), 0)
    lane = lax.broadcasted_iota(jnp.int32, (3 * choices, LANES), 1)
    placed = lax.dot_general(
        notes.astype(jnp.bfloat16),
        jnp.where(kind == lane, 1.0, 0.0).astype(jnp.bfloat16),
        (((0,), (0,)), ((), ())),
        preferred_element_type=jnp.float32,
    )
    out_ref[:, width:] = placed.astype(jnp.bfloat16)
    copies[3].wait()


def picks_kernel(expert_ref, *refs, capacity, choices, tok_rows):
    blocks, (rows_ref, mix_ref) = refs[:-2], refs[-2:]
    count, width = blocks[0].shape[0], rows_ref.shape[1]
    slots = mix_ref.shape[2]
    token = lax.broadcasted_iota(jnp.int32, (count, slots), 0)
    slot = lax.broadcasted_iota(jnp.int32, (count, slots), 1)
    wanted = (expert_ref[0] * capacity + slot % capacity).astype(jnp.float32)
    here = slot // capacity == token // tok_rows
    for j, block in enumerate(blocks):
        notes = block[:, width:].astype(jnp.float32)
        experts, places = notes[:, :choices], notes[:, choices : 2 * choices]
        code = jnp.where(places < capacity, experts * capacity + places, -1.0)
        weight = jnp.zeros((count, slots), jnp.float32)
        found = jnp.zeros((count, slots), jnp.float32)
        for k in range(choices):
            value = notes[:, 2 * choices + k : 2 * choices + k + 1]
            match = here & (code[:, k : k + 1] == wanted)
            found = jnp.where(match, 1.0, found)
            weight = jnp.where(match, value, weight)
        rows = lax.dot_general(
            found.astype(jnp.bfloat16),
            block[:, :width],
            (((0,), (0,)), ((), ())),
            preferred_element_type=jnp.float32,
        )
        rows_ref[j * slots : (j + 1) * slots, :] = rows.astype(jnp.bfloat16)
        mix_ref[j] = weight.astype(jnp.bfloat16)


def shared_kernel(*refs):
    blocks, (gate_ref, gate_up_hbm, down_hbm, out_ref, gate_up, down, sems) = refs[:-7], refs[-7:]
    fetch_in = pltpu.make_async_copy(gate_up_hbm, gate_up, sems.at[0])
    fetch_out = pltpu.make_async_copy(down_hbm, down, sems.at[1])
    fetch_in.start()
    fetch_out.start()
    count, width = blocks[0].shape[0], out_ref.shape[2]
    gate_row = gate_ref[...].astype(jnp.float32)
    scales = []
    for block in blocks:
        score = jnp.sum(block[:, :width].astype(jnp.float32) * gate_row, axis=1, keepdims=True)
        scales.append(1.0 / (1.0 + jnp.exp(-score)))
    tokens = jnp.concatenate([block[:, :width] for block in blocks])
    contract = (((1,), (1,)), ((), ()))
    fetch_in.wait()
    gate = lax.dot_general(tokens, gate_up[0], contract, preferred_element_type=jnp.float32)
    up = lax.dot_general(tokens, gate_up[1], contract, preferred_element_type=jnp.float32)
    hidden = (gate / (1.0 + jnp.exp(-gate)) * up).astype(jnp.bfloat16)
    fetch_out.wait()
    for j, scale in enumerate(scales):
        part = hidden[j * count : (j + 1) * count]
        out_ref[j] = scale * jnp.dot(part, down[...], preferred_element_type=jnp.float32)


def combine_kernel(kept_ref, got_ref, mix_ref, shared_ref, own_ref, *sent_refs):
    rows = (kept_ref[...] + got_ref[...].astype(jnp.float32)).astype(jnp.bfloat16)
    slots = mix_ref.shape[2]
    for j, out_ref in enumerate((own_ref, *sent_refs)):
        part = rows[j * slots : (j + 1) * slots]
        routed = jnp.dot(mix_ref[j], part, preferred_element_type=jnp.float32)
        out_ref[...] = (shared_ref[j] + routed).astype(out_ref.dtype)


def in_vmem(count):
    return [pl.BlockSpec(memory_space=pltpu.VMEM)] * count


def on_device(
    tokens,
    expert_ids,
    slot_index,
    route_weight,
    shared_gate,
    shared_gate_up,
    shared_down,
    expert_gate_up,
    expert_down,
):
    planes = lax.axis_size("plane")
    tok_rows, width = tokens.shape
    choices = expert_ids.shape[1]
    capacity = max(2, tok_rows * choices // planes)
    near = 4
    count = planes // near * tok_rows
    slots = planes // near * capacity
    units = shared_down.shape[0]
    anywhere = pl.BlockSpec(memory_space=pl.ANY)
    small = pltpu.CompilerParams(vmem_limit_bytes=GLUE_VMEM)

    noted = pl.pallas_call(
        notes_kernel,
        out_shape=jax.ShapeDtypeStruct((tok_rows, width + LANES), jnp.bfloat16),
        in_specs=[pl.BlockSpec(memory_space=pltpu.HBM)] * 4,
        out_specs=in_vmem(1)[0],
        scratch_shapes=[
            pltpu.VMEM((choices, tok_rows), jnp.int32),
            pltpu.VMEM((choices, tok_rows), jnp.int32),
            pltpu.VMEM((choices, tok_rows), jnp.bfloat16),
            pltpu.SemaphoreType.DMA((4,)),
        ],
        compiler_params=pltpu.CompilerParams(vmem_limit_bytes=64 << 20),
    )(tokens, expert_ids.T, slot_index.T, route_weight.T)
    blocks = gather_planes(noted, near)

    expert = lax.axis_index("plane").astype(jnp.int32).reshape(1)
    rows, mix = pl.pallas_call(
        functools.partial(
            picks_kernel, capacity=capacity, choices=choices, tok_rows=tok_rows
        ),
        out_shape=(
            jax.ShapeDtypeStruct((near * slots, width), jnp.bfloat16),
            jax.ShapeDtypeStruct((near, count, slots), jnp.bfloat16),
        ),
        in_specs=[pl.BlockSpec(memory_space=pltpu.SMEM)] + in_vmem(near),
        out_specs=tuple(in_vmem(2)),
        compiler_params=small,
    )(expert, *blocks)

    gate_up, down = expert_gate_up[0].swapaxes(1, 2), expert_down[0]
    gate_up_chip = from_chip(gate_up, weight_partner)
    down_chip = from_chip(down, weight_partner)
    gate_up_core, down_core = from_core(gate_up), from_core(down)
    gate_up_far = from_core(gate_up_chip)
    down_far = from_core(down_chip)
    other_rows = from_chip(rows, row_partner)
    kept, sent = expert_partials(
        rows,
        other_rows,
        (gate_up, gate_up_core, gate_up_far, gate_up_chip),
        (down, down_core, down_far, down_chip),
    )
    got = from_chip(sent, row_partner)

    shared_part = pl.pallas_call(
        shared_kernel,
        out_shape=jax.ShapeDtypeStruct((near, count, width), jnp.float32),
        in_specs=in_vmem(near + 1) + [anywhere] * 2,
        out_specs=in_vmem(1)[0],
        scratch_shapes=[
            pltpu.VMEM((2, units, width), jnp.bfloat16),
            pltpu.VMEM((units, width), jnp.bfloat16),
            pltpu.SemaphoreType.DMA((2,)),
        ],
        compiler_params=pltpu.CompilerParams(vmem_limit_bytes=KERNEL_VMEM),
        cost_estimate=pl.CostEstimate(
            flops=6 * near * count * width * units,
            bytes_accessed=6 * units * width,
            transcendentals=near * count * units,
        ),
    )(*blocks, shared_gate.reshape(1, width), shared_gate_up.swapaxes(1, 2), shared_down)

    own, *others = pl.pallas_call(
        combine_kernel,
        out_shape=[jax.ShapeDtypeStruct((count, width), jnp.float32)]
        + [jax.ShapeDtypeStruct((count, width), jnp.bfloat16)] * (near - 1),
        in_specs=in_vmem(4),
        out_specs=in_vmem(near),
        compiler_params=small,
    )(kept, got, mix, shared_part)
    return reduce_planes(own, others, near, tok_rows).astype(jnp.bfloat16)


def solution(mesh):
    in_specs = (
        P(("groups", "plane", "depth", "tok"), None),
        P(("groups", "plane", "depth", "tok"), None),
        P(("groups", "plane", "depth", "tok"), None),
        P(("groups", "plane", "depth", "tok"), None),
        P(),
        P(None, None, "plane"),
        P("plane", None),
        P("plane", None, None, ("depth", "tok")),
        P("plane", ("depth", "tok"), None),
    )
    out_specs = P(("groups", "plane", "depth", "tok"), None)
    return jax.shard_map(on_device, mesh=mesh, in_specs=in_specs, out_specs=out_specs, check_vma=False)
```
